512 devices in a mesh: grp: 2 (over y), col: 16 (over z), slc: 8 (over x), bat: 2 (over core).
Axes of the slice: x: 8, y: 2, z: 16, core: 2. Of those that a mesh axis runs over, the one named last changes fastest.
The devices are a block of a 8x8x16 slice.
Arguments:
- site_tensors: bfloat16 [16, 288, 2, 64, 128], P(('grp', 'slc'), 'col'), parts along dimension 0, may hold values from -1.2 to 1.2
- left_edge: float32 [16, 64, 128], P(('grp', 'slc')), parts along dimension 0, may hold values from -0.5 to 0.5
- right_edge: float32 [16, 64, 128], P(('grp', 'slc')), parts along dimension 0, may hold values from -0.5 to 0.5
- order: int32 [576], P(('grp', 'col')), parts along dimension 0, may hold values from 0 to 287, each once
- bitstrings: int32 [128, 288], P(('grp', 'bat')), parts along dimension 0, may hold values 0 or 1
Outputs:
- amplitudes: float32 [2, 128], P(None, ('grp', 'bat')), parts along dimension 1
The draws below stay inside these ranges and needn't reach their ends.
There are 2 independent parts, one for each index of `grp`. The reference program is written for one: setup_inputs(seed, part) draws one part's arguments, and reference() takes and returns one part's arrays. A program takes and returns all parts, laid end to end along the dimension named above; each array names one. Nothing has to cross between parts.
Inputs may be any that keep to these rules, and one draw needn't show every extreme that they name: `order`: a permutation of the 288 qubit indices.
All inputs are finite; a program needn't handle non-finite values. No bound on the sum of `bitstrings` on one device may be relied on, other than what follows from the above.
Results may differ from the reference program's by a relative error of at most 0.0003.
Values sent between devices are 32-bit elements; how exact they have to be, the bound alone decides.
No kernel may reach another device: no remote copies, remote signals or barrier semaphores. Data moves between devices by JAX's collectives and lax.ppermute only.
A program may use at most 64 MiB of HBM per device.

```python
import math
import jax
import jax.numpy as jnp
from jax import lax

CHI = 64
NQ = 288
BITS = 64
SLICES = 8


def batch_product(left_factor, right_factor):
    return jnp.einsum('nij,njk->nik', left_factor, right_factor, precision=lax.Precision.HIGHEST)


def complex_batch(left_real, left_imag, right_real, right_imag):
    real_part = batch_product(left_real, right_real) - batch_product(left_imag, right_imag)
    imag_part = batch_product(left_real, right_imag) + batch_product(left_imag, right_real)
    return (real_part, imag_part)


def draw_site_tensors(key, part):
    matrix_count = SLICES * NQ * 2
    subkeys = jax.random.split(jax.random.fold_in(key, 7103), 3)
    shape = (matrix_count, CHI, CHI)
    spread = math.sqrt(1.0 / (2.0 * CHI))
    noise_real = jax.random.normal(subkeys[0], shape, jnp.float32) * spread
    noise_imag = jax.random.normal(subkeys[1], shape, jnp.float32) * spread
    unit_matrix = jnp.eye(CHI, dtype=jnp.float32)
    current_real = (2.0 * unit_matrix[None] + noise_real) / 3.2
    current_imag = noise_imag / 3.2
    for sweep_index in range(10):
        adjoint_real = jnp.swapaxes(current_real, 1, 2)
        adjoint_imag = -jnp.swapaxes(current_imag, 1, 2)
        gram_real, gram_imag = complex_batch(adjoint_real, adjoint_imag, current_real, current_imag)
        cubic_real, cubic_imag = complex_batch(current_real, current_imag, gram_real, gram_imag)
        current_real = 1.5 * current_real - 0.5 * cubic_real
        current_imag = 1.5 * current_imag - 0.5 * cubic_imag
    matrix_gain = jnp.exp(jax.random.uniform(subkeys[2], (matrix_count, 1, 1), jnp.float32, -0.05, 0.05))
    current_real = current_real * matrix_gain
    current_imag = current_imag * matrix_gain
    joined = jnp.concatenate([current_real, current_imag], axis=-1)
    return joined.reshape(SLICES, NQ, 2, CHI, 2 * CHI).astype(jnp.bfloat16)


def plant(drawn, rng, smallest, high):
    dims = drawn.shape
    place = [jax.random.randint(jax.random.fold_in(rng, axis), (), 0, dims[axis]) for axis in range(len(dims))]
    drawn = drawn.at[tuple(place)].set(smallest)
    longest = dims.index(max(dims))
    place[longest] = (place[longest] + 1) % dims[longest]
    return drawn.at[tuple(place)].set(high)


def block_levels(key, shape, pieces, least, high):
    level, own = 1.0, jax.random.fold_in(key, 6)
    for axis_at, shards_of in pieces:
        draws = jnp.exp(jax.random.uniform(jax.random.fold_in(own, axis_at), (shards_of,), jnp.float32, least / len(pieces), high / len(pieces)))
        level = level * jnp.repeat(draws, shape[axis_at] // shards_of).reshape([-1 if axis == axis_at else 1 for axis in range(len(shape))])
    return level


def normal_values(stream_key, shape, deviation, most, cuts=(), kind=jnp.bfloat16):
    result = jax.random.normal(stream_key, shape, jnp.float32) * deviation
    if len(cuts) > 0:
        result = block_levels(stream_key, shape, cuts, -0.22, 0.18) * result
    return jnp.clip(result, min=-most, max=most).astype(kind)


def setup_inputs(seed: int = 0, part: int = 0) -> dict:
    key_of = jax.random.split(jax.random.key(seed), 6)
    part_keys = jax.random.split(jax.random.fold_in(key_of[5], part), 6)
    return {
        "site_tensors": draw_site_tensors(jax.random.fold_in(jax.random.fold_in(key_of[5], part), 71), part),
        "left_edge": normal_values(part_keys[1], (SLICES, CHI, 2 * CHI), (2 * CHI) ** -0.5, 0.5, ((0, 8),), jnp.float32),
        "right_edge": normal_values(part_keys[2], (SLICES, CHI, 2 * CHI), (2 * CHI) ** -0.5, 0.5, ((0, 8),), jnp.float32),
        "order": jax.random.permutation(part_keys[3], NQ).astype(jnp.int32),
        "bitstrings": plant((jax.random.randint(part_keys[4], (BITS, NQ), 0, 2) < 1).astype(jnp.int32), jax.random.fold_in(part_keys[4], 1), 0, 1),
    }


def rotate(block):
    middle = block.shape[-1] // 2
    return jnp.concatenate([-block[..., middle:], block[..., :middle]], axis=-1)


def complex_product(first_factor, second_factor):
    stacked = jnp.concatenate([second_factor, rotate(second_factor)], axis=-2)
    return jnp.einsum("bij,bjk->bik", first_factor, stacked, precision=lax.Precision.HIGHEST)


def closing(boundary, edge):
    real_left = boundary[..., :CHI]
    imag_left = boundary[..., CHI:]
    real_right = edge[..., :CHI]
    imag_right = edge[..., CHI:]
    real_part = jnp.sum(real_left * real_right - imag_left * imag_right, axis=(1, 2))
    imag_part = jnp.sum(real_left * imag_right + imag_left * real_right, axis=(1, 2))
    return jnp.stack([real_part, imag_part])


def slice_amplitude(operands, site_bits):
    tensors, left_start, right_stop = operands
    opening = jnp.broadcast_to(left_start, (BITS, CHI, 2 * CHI)).astype(jnp.float32)

    def advance(boundary, site_item):
        matrices, chosen_bits = site_item
        matrices = matrices.astype(jnp.float32)
        chosen = jnp.where(chosen_bits[:, None, None] == 1, matrices[1], matrices[0])
        return complex_product(boundary, chosen), None

    final_state, unused = lax.scan(advance, opening, (tensors, site_bits))
    return closing(final_state, right_stop)


def reference(site_tensors, left_edge, right_edge, order, bitstrings):
    site_bits = jnp.take(bitstrings, order.astype(jnp.int32), axis=1).T
    per_slice = lax.map(lambda operands: slice_amplitude(operands, site_bits), (site_tensors, left_edge, right_edge))
    return jnp.sum(per_slice, axis=0)
```

```python
import functools

import jax
import jax.numpy as jnp
from jax import lax
from jax.experimental import pallas as pl
from jax.experimental.pallas import tpu as pltpu
from jax.sharding import Mesh, PartitionSpec as P

F32 = jnp.float32
BF16 = jnp.bfloat16
BLOCK = 4
PREFIX = 4
PARAMS = pltpu.CompilerParams(vmem_limit_bytes=16 * 1024 * 1024)


def lane_sign(rows, width):
    lane = lax.broadcasted_iota(jnp.int32, (rows, width), 1)
    return jnp.where(lane < width // 2, -1.0, 1.0).astype(F32)


def rotated(block, sign):
    return pltpu.roll(block, block.shape[1] // 2, 1) * sign


def split(value):
    high = value.astype(BF16)
    low = (value - high.astype(F32)).astype(BF16)
    return high, low


def dot(a, b):
    return jnp.dot(a, b, preferred_element_type=F32)


def pair_product(first, second, sign):
    width = first.shape[1]
    first_high, first_low = split(first)
    second_high, second_low = split(jnp.concatenate([second, rotated(second, sign)], axis=0))
    half = jnp.concatenate([second_high, second_low], axis=1)
    both = dot(
        jnp.concatenate([first_high, first_low], axis=1),
        jnp.concatenate([half, half], axis=0),
    )
    return both[:, :width] + both[:, width:]


def opening_matrix(left, right, sign):
    bond, width = left.shape
    left_high, left_low = split(left)
    right_high, right_low = split(right)
    gram = lax.dot_general(
        jnp.concatenate([right_high, right_high, right_low, right_low], axis=0),
        jnp.concatenate([left_high, left_low, left_high, left_low], axis=0),
        (((0,), (0,)), ((), ())),
        preferred_element_type=F32,
    )
    return gram[:bond] + rotated(gram[bond:], sign)


def column_kernel(base, order_ref, bits_ref, role_ref, tensors_ref, left_ref, right_ref, out_ref, state_ref, table_ref):
    sites, _, bond, width = tensors_ref.shape
    slots = out_ref.shape[0]
    sign = lane_sign(bond, width)
    mask = role_ref[0]
    first = role_ref[1] == 1
    row = lax.broadcasted_iota(jnp.int32, (bond, width), 0)
    lane = lax.broadcasted_iota(jnp.int32, (bond, width), 1)
    unit = jnp.where(row == lane, 1.0, 0.0).astype(F32)
    opening = jnp.where(first, opening_matrix(left_ref[...], right_ref[...], sign), unit)

    def weights(site):
        halves = []
        for value in range(2):
            tensor = tensors_ref[site, value].astype(F32)
            halves.append(jnp.concatenate([tensor, rotated(tensor, sign)], axis=0).astype(BF16))
        half = jnp.concatenate(halves, axis=1)
        return jnp.concatenate([half, half], axis=0)

    def bit(site, slot):
        return bits_ref[(base + slot) ^ mask, order_ref[site]]

    table = opening
    for site in range(PREFIX):
        high, low = split(table)
        both = dot(jnp.concatenate([high, low], axis=1), weights(site))
        table = jnp.concatenate([both[:, :width], both[:, width:]], axis=0)
    high, low = split(table)
    table_ref[:, :width] = high
    table_ref[:, width:] = low
    for slot in range(slots):
        entry = bit(0, slot)
        for site in range(1, PREFIX):
            entry = entry + bit(site, slot) * (1 << site)
        start = pl.multiple_of(entry * bond, bond)
        state_ref[slot * bond:(slot + 1) * bond, :] = table_ref[pl.ds(start, bond), :]

    for site in range(PREFIX, sites):
        matrix = weights(site)
        for start in range(0, slots, BLOCK):
            both = dot(state_ref[start * bond:(start + BLOCK) * bond, :], matrix)
            for slot in range(start, start + BLOCK):
                part = both[(slot - start) * bond:(slot - start + 1) * bond]
                value = jnp.where(bit(site, slot) == 1, part[:, width:], part[:, :width])
                if site == sites - 1:
                    out_ref[slot] = value
                else:
                    high, low = split(value)
                    state_ref[slot * bond:(slot + 1) * bond, :width] = high
                    state_ref[slot * bond:(slot + 1) * bond, width:] = low


def column_products(base, slots, order, bits, role, tensors, left, right):
    sites, _, bond, width = tensors.shape
    scalar = pl.BlockSpec(memory_space=pltpu.SMEM)
    vector = pl.BlockSpec(memory_space=pltpu.VMEM)
    return pl.pallas_call(
        functools.partial(column_kernel, base),
        out_shape=jax.ShapeDtypeStruct((slots, bond, width), F32),
        in_specs=[scalar, scalar, scalar, vector, vector, vector],
        out_specs=vector,
        scratch_shapes=[
            pltpu.VMEM((slots * bond, 2 * width), BF16),
            pltpu.VMEM(((1 << PREFIX) * bond, 2 * width), BF16),
        ],
        cost_estimate=pl.CostEstimate(
            flops=sites * slots * bond * (2 * width) ** 2, bytes_accessed=slots * bond * width * 8, transcendentals=0
        ),
        compiler_params=PARAMS,
        name="column_products",
    )(order, bits, role, tensors, left, right)


def joined(flag, kept, received, sign):
    before = jnp.where(flag, received, kept)
    after = jnp.where(flag, kept, received)
    return pair_product(before, after, sign)


def join_kernel(role_ref, kept_ref, received_ref, *out_refs):
    items, bond, width = kept_ref.shape
    sign = lane_sign(bond, width)
    flag = role_ref[0] == 1
    per = out_refs[0].shape[0]
    for item in range(items):
        out_refs[item // per][item % per] = joined(flag, kept_ref[item], received_ref[item], sign)


def join(flag, kept, received, outs):
    items, bond, width = kept.shape
    out = jax.ShapeDtypeStruct((items // outs, bond, width), F32)
    vector = pl.BlockSpec(memory_space=pltpu.VMEM)
    return pl.pallas_call(
        join_kernel,
        out_shape=(out,) * outs,
        in_specs=[pl.BlockSpec(memory_space=pltpu.SMEM), vector, vector],
        out_specs=(vector,) * outs,
        compiler_params=PARAMS,
        name="join",
    )(flag, kept, received)


def close_kernel(role_ref, parts_ref, out_ref):
    groups, items, bond, width = parts_ref.shape
    sign = lane_sign(bond, width)
    row = lax.broadcasted_iota(jnp.int32, (bond, width), 0)
    lane = lax.broadcasted_iota(jnp.int32, (bond, width), 1)
    slot = lax.broadcasted_iota(jnp.int32, out_ref.shape, 1)
    which = lax.broadcasted_iota(jnp.int32, out_ref.shape, 0)
    total = jnp.zeros(out_ref.shape, F32)
    for item in range(items):
        chain = [parts_ref[group, item] for group in range(groups)]
        while len(chain) > 1:
            chain = [pair_product(chain[k], chain[k + 1], sign) for k in range(0, len(chain), 2)]
        real = jnp.sum(jnp.where(row == lane, chain[0], 0.0), keepdims=True)
        imag = jnp.sum(jnp.where(row + bond == lane, chain[0], 0.0), keepdims=True)
        value = jnp.where(which == 0, real, imag)
        total = jnp.where(slot == (role_ref[0] ^ item), value, total)
    out_ref[...] = total


def close(base, parts, rows):
    return pl.pallas_call(
        close_kernel,
        out_shape=jax.ShapeDtypeStruct((2, rows), F32),
        in_specs=[pl.BlockSpec(memory_space=pltpu.SMEM), pl.BlockSpec(memory_space=pltpu.VMEM)],
        out_specs=pl.BlockSpec(memory_space=pltpu.VMEM),
        compiler_params=PARAMS,
        name="close",
    )(base, parts)


def shift_of(core, cols):
    return (core * 3) % cols


def partner_pairs(cols, cores, distance):
    pairs = []
    for core in range(cores):
        shift = shift_of(core, cols)
        for col in range(cols):
            role = (col - shift) % cols
            other = ((role ^ distance) + shift) % cols
            pairs.append((col * cores + core, other * cores + core))
    return pairs


def solution(mesh):
    shape = dict(mesh.shape)
    inner = 4
    outer = shape["col"] // inner
    cores = shape["bat"]
    cols = shape["col"]
    fine = Mesh(
        mesh.devices.reshape(shape["grp"], outer, inner, shape["slc"], cores),
        ("grp", "far", "near", "slc", "bat"),
    )

    def on_device(site_tensors, left_edge, right_edge, order, bitstrings):
        rows = bitstrings.shape[0]
        core = lax.axis_index("bat")
        far = lax.axis_index("far")
        col = far * inner + lax.axis_index("near")
        role = (col - shift_of(core, cols) + cols) % cols
        bit0, bit1 = role & 1, (role >> 1) & 1
        mask = bit0 * (rows // 2) + bit1 * (rows // 4)
        first = (col == 0).astype(jnp.int32)
        operands = (order, bitstrings, jnp.stack([mask, first]), site_tensors[0], left_edge[0], right_edge[0])
        sent = column_products(rows // 2, rows // 2, *operands)
        kept = column_products(0, rows // 2, *operands)
        received = lax.ppermute(sent, ("far", "near", "bat"), partner_pairs(cols, cores, 1))
        kept, sent = join(bit0[None], kept, received, 2)
        received = lax.ppermute(sent, ("far", "near", "bat"), partner_pairs(cols, cores, 2))
        (quad,) = join(bit1[None], kept, received, 1)
        items, bond, width = quad.shape
        per = items // outer
        parts = lax.all_to_all(
            quad.reshape(outer, per, bond, width), "far", split_axis=0, concat_axis=0, tiled=True
        )
        base = mask ^ (far * per)
        placed = close(base[None], parts, rows)
        everyone = outer * inner * shape["slc"]
        spread = jnp.broadcast_to(placed, (everyone, 2, rows))
        gathered = lax.all_to_all(spread, ("far", "near", "slc"), split_axis=0, concat_axis=0, tiled=True)
        return jnp.sum(gathered, axis=0)

    return jax.shard_map(
        on_device,
        mesh=fine,
        in_specs=(
            P(("grp", "slc"), ("far", "near"), None, None, None),
            P(("grp", "slc"), None, None),
            P(("grp", "slc"), None, None),
            P(("grp", "far", "near")),
            P(("grp", "bat"), None),
        ),
        out_specs=P(None, ("grp", "bat")),
        check_vma=False,
    )
```

```python
import functools

import jax
import jax.numpy as jnp
from jax import lax
from jax.experimental import pallas as pl
from jax.experimental.pallas import tpu as pltpu
from jax.sharding import Mesh, PartitionSpec as P

F32 = jnp.float32
BF16 = jnp.bfloat16
BLOCK = 4
PREFIX = 4
PARAMS = pltpu.CompilerParams(vmem_limit_bytes=16 * 1024 * 1024)


def lane_sign(rows, width):
    lane = lax.broadcasted_iota(jnp.int32, (rows, width), 1)
    return jnp.where(lane < width // 2, -1.0, 1.0).astype(F32)


def rotated(block, sign):
    return pltpu.roll(block, block.shape[1] // 2, 1) * sign


def split(value):
    high = value.astype(BF16)
    low = (value - high.astype(F32)).astype(BF16)
    return high, low


def dot(a, b):
    return jnp.dot(a, b, preferred_element_type=F32)


def pair_product(first, second, sign):
    width = first.shape[1]
    first_high, first_low = split(first)
    second_high, second_low = split(jnp.concatenate([second, rotated(second, sign)], axis=0))
    half = jnp.concatenate([second_high, second_low], axis=1)
    both = dot(
        jnp.concatenate([first_high, first_low], axis=1),
        jnp.concatenate([half, half], axis=0),
    )
    return both[:, :width] + both[:, width:]


def opening_matrix(left, right, sign):
    bond, width = left.shape
    left_high, left_low = split(left)
    right_high, right_low = split(right)
    gram = lax.dot_general(
        jnp.concatenate([right_high, right_high, right_low, right_low], axis=0),
        jnp.concatenate([left_high, left_low, left_high, left_low], axis=0),
        (((0,), (0,)), ((), ())),
        preferred_element_type=F32,
    )
    return gram[:bond] + rotated(gram[bond:], sign)


def column_kernel(
    base, order_ref, role_ref, bits_hbm, tensors_hbm, left_hbm, right_hbm, out_ref,
    bits_ref, tensors_ref, left_ref, right_ref, state_ref, table_ref, start_ref, word_ref, words_ref, arrived,
):
    sites, _, bond, width = tensors_ref.shape
    slots = out_ref.shape[0]
    copies = [
        pltpu.make_async_copy(source, target, arrived.at[index])
        for index, (source, target) in enumerate(
            (
                (bits_hbm, bits_ref),
                (tensors_hbm.at[pl.ds(0, PREFIX)], tensors_ref.at[pl.ds(0, PREFIX)]),
                (tensors_hbm.at[pl.ds(PREFIX, sites - PREFIX)], tensors_ref.at[pl.ds(PREFIX, sites - PREFIX)]),
            )
        )
    ]
    for copy in copies:
        copy.start()
    sign = lane_sign(bond, width)
    mask = role_ref[0]
    qubit = lax.broadcasted_iota(jnp.int32, (8, bits_ref.shape[1]), 1)
    place = jnp.zeros(qubit.shape, F32)
    for site in range(sites):
        place = jnp.where(qubit == order_ref[site], float(1 << site), place)
    place = place.astype(BF16)

    def weights(site):
        halves = []
        for value in range(2):
            tensor = tensors_ref[site, value].astype(F32)
            halves.append(jnp.concatenate([tensor, rotated(tensor, sign)], axis=0).astype(BF16))
        half = jnp.concatenate(halves, axis=1)
        return jnp.concatenate([half, half], axis=0)

    copies[0].wait()
    word = lax.dot_general(
        place, bits_ref[...].astype(F32).astype(BF16), (((1,), (1,)), ((), ())), preferred_element_type=F32
    )
    word_ref[...] = jnp.zeros(word_ref.shape, jnp.int32)
    word_ref[:, :word.shape[1]] = word.astype(jnp.int32)
    to_scalars = pltpu.make_async_copy(word_ref, words_ref, arrived.at[len(copies)])
    to_scalars.start()

    copies[1].wait()
    for value in range(2):
        start_ref[value * bond:(value + 1) * bond, :width] = tensors_ref[0, value]
    start_ref[:, width:] = jnp.zeros((2 * bond, width), BF16)

    @pl.when(role_ref[1] == 1)
    def _():
        edges = [
            pltpu.make_async_copy(left_hbm, left_ref, arrived.at[len(copies) + 1]),
            pltpu.make_async_copy(right_hbm, right_ref, arrived.at[len(copies) + 2]),
        ]
        for edge in edges:
            edge.start()
        for edge in edges:
            edge.wait()
        high, low = split(opening_matrix(left_ref[...], right_ref[...], sign))
        both = dot(jnp.concatenate([high, low], axis=1), weights(0))
        high, low = split(jnp.concatenate([both[:, :width], both[:, width:]], axis=0))
        start_ref[:, :width] = high
        start_ref[:, width:] = low

    operand = start_ref[...]
    for site in range(1, PREFIX):
        both = dot(operand, weights(site))
        high, low = split(jnp.concatenate([both[:, :width], both[:, width:]], axis=0))
        operand = jnp.concatenate([high, low], axis=1)
    table_ref[...] = operand
    to_scalars.wait()
    words = [words_ref[0, (base + slot) ^ mask] for slot in range(slots)]
    for slot in range(slots):
        start = pl.multiple_of((words[slot] & ((1 << PREFIX) - 1)) * bond, bond)
        state_ref[slot * bond:(slot + 1) * bond, :] = table_ref[pl.ds(start, bond), :]

    copies[2].wait()
    for site in range(PREFIX, sites):
        matrix = weights(site)
        for start in range(0, slots, BLOCK):
            both = dot(state_ref[start * bond:(start + BLOCK) * bond, :], matrix)
            for slot in range(start, start + BLOCK):
                part = both[(slot - start) * bond:(slot - start + 1) * bond]
                value = jnp.where((words[slot] & (1 << site)) != 0, part[:, width:], part[:, :width])
                if site == sites - 1:
                    out_ref[slot] = value
                else:
                    high, low = split(value)
                    state_ref[slot * bond:(slot + 1) * bond, :width] = high
                    state_ref[slot * bond:(slot + 1) * bond, width:] = low


def column_products(base, slots, order, bits, role, tensors, left, right):
    sites, _, bond, width = tensors.shape
    scalar = pl.BlockSpec(memory_space=pltpu.SMEM)
    far = pl.BlockSpec(memory_space=pltpu.HBM)
    return pl.pallas_call(
        functools.partial(column_kernel, base),
        out_shape=jax.ShapeDtypeStruct((slots, bond, width), F32),
        in_specs=[scalar, scalar, far, far, far, far],
        out_specs=pl.BlockSpec(memory_space=pltpu.VMEM),
        scratch_shapes=[
            pltpu.VMEM(bits.shape, jnp.int32),
            pltpu.VMEM(tensors.shape, BF16),
            pltpu.VMEM((bond, width), F32),
            pltpu.VMEM((bond, width), F32),
            pltpu.VMEM((slots * bond, 2 * width), BF16),
            pltpu.VMEM(((1 << PREFIX) * bond, 2 * width), BF16),
            pltpu.VMEM((2 * bond, 2 * width), BF16),
            pltpu.VMEM((8, width), jnp.int32),
            pltpu.SMEM((8, width), jnp.int32),
            pltpu.SemaphoreType.DMA((6,)),
        ],
        cost_estimate=pl.CostEstimate(
            flops=sites * slots * bond * (2 * width) ** 2, bytes_accessed=slots * bond * width * 8, transcendentals=0
        ),
        compiler_params=PARAMS,
        name="column_products",
    )(order, role, *(pltpu.with_memory_space_constraint(a, pltpu.HBM) for a in (bits, tensors, left, right)))


def joined(flag, kept, received, sign):
    before = jnp.where(flag, received, kept)
    after = jnp.where(flag, kept, received)
    return pair_product(before, after, sign)


def join_kernel(role_ref, kept_ref, received_ref, *out_refs):
    items, bond, width = kept_ref.shape
    sign = lane_sign(bond, width)
    flag = role_ref[0] == 1
    per = out_refs[0].shape[0]
    for item in range(items):
        out_refs[item // per][item % per] = joined(flag, kept_ref[item], received_ref[item], sign)


def join(flag, kept, received, outs):
    items, bond, width = kept.shape
    out = jax.ShapeDtypeStruct((items // outs, bond, width), F32)
    vector = pl.BlockSpec(memory_space=pltpu.VMEM)
    return pl.pallas_call(
        join_kernel,
        out_shape=(out,) * outs,
        in_specs=[pl.BlockSpec(memory_space=pltpu.SMEM), vector, vector],
        out_specs=(vector,) * outs,
        compiler_params=PARAMS,
        name="join",
    )(flag, kept, received)


def close_kernel(role_ref, parts_ref, out_ref):
    groups, items, bond, width = parts_ref.shape
    sign = lane_sign(bond, width)
    row = lax.broadcasted_iota(jnp.int32, (bond, width), 0)
    lane = lax.broadcasted_iota(jnp.int32, (bond, width), 1)
    slot = lax.broadcasted_iota(jnp.int32, out_ref.shape, 1)
    which = lax.broadcasted_iota(jnp.int32, out_ref.shape, 0)
    total = jnp.zeros(out_ref.shape, F32)
    for item in range(items):
        chain = [parts_ref[group, item] for group in range(groups)]
        while len(chain) > 1:
            chain = [pair_product(chain[k], chain[k + 1], sign) for k in range(0, len(chain), 2)]
        real = jnp.sum(jnp.where(row == lane, chain[0], 0.0), keepdims=True)
        imag = jnp.sum(jnp.where(row + bond == lane, chain[0], 0.0), keepdims=True)
        value = jnp.where(which == 0, real, imag)
        total = jnp.where(slot == (role_ref[0] ^ item), value, total)
    out_ref[...] = total


def close(base, parts, rows):
    return pl.pallas_call(
        close_kernel,
        out_shape=jax.ShapeDtypeStruct((2, rows), F32),
        in_specs=[pl.BlockSpec(memory_space=pltpu.SMEM), pl.BlockSpec(memory_space=pltpu.VMEM)],
        out_specs=pl.BlockSpec(memory_space=pltpu.VMEM),
        compiler_params=PARAMS,
        name="close",
    )(base, parts)


def shift_of(core, cols):
    return (core * 3) % cols


def partner_pairs(cols, cores, distance):
    pairs = []
    for core in range(cores):
        shift = shift_of(core, cols)
        for col in range(cols):
            role = (col - shift) % cols
            other = ((role ^ distance) + shift) % cols
            pairs.append((col * cores + core, other * cores + core))
    return pairs


def solution(mesh):
    shape = dict(mesh.shape)
    inner = 4
    outer = shape["col"] // inner
    cores = shape["bat"]
    cols = shape["col"]
    fine = Mesh(
        mesh.devices.reshape(shape["grp"], outer, inner, shape["slc"], cores),
        ("grp", "far", "near", "slc", "bat"),
    )

    def on_device(site_tensors, left_edge, right_edge, order, bitstrings):
        rows = bitstrings.shape[0]
        core = lax.axis_index("bat")
        far = lax.axis_index("far")
        col = far * inner + lax.axis_index("near")
        role = (col - shift_of(core, cols) + cols) % cols
        bit0, bit1 = role & 1, (role >> 1) & 1
        mask = bit0 * (rows // 2) + bit1 * (rows // 4)
        first = (col == 0).astype(jnp.int32)
        operands = (order, bitstrings, jnp.stack([mask, first]), site_tensors[0], left_edge[0], right_edge[0])
        sent = column_products(rows // 2, rows // 2, *operands)
        kept = column_products(0, rows // 2, *operands)
        received = lax.ppermute(sent, ("far", "near", "bat"), partner_pairs(cols, cores, 1))
        kept, sent = join(bit0[None], kept, received, 2)
        received = lax.ppermute(sent, ("far", "near", "bat"), partner_pairs(cols, cores, 2))
        (quad,) = join(bit1[None], kept, received, 1)
        items, bond, width = quad.shape
        per = items // outer
        parts = lax.all_to_all(
            quad.reshape(outer, per, bond, width), "far", split_axis=0, concat_axis=0, tiled=True
        )
        base = mask ^ (far * per)
        placed = close(base[None], parts, rows)
        everyone = outer * inner * shape["slc"]
        spread = jnp.broadcast_to(placed, (everyone, 2, rows))
        gathered = lax.all_to_all(spread, ("far", "near", "slc"), split_axis=0, concat_axis=0, tiled=True)
        return jnp.sum(gathered, axis=0)

    return jax.shard_map(
        on_device,
        mesh=fine,
        in_specs=(
            P(("grp", "slc"), ("far", "near"), None, None, None),
            P(("grp", "slc"), None, None),
            P(("grp", "slc"), None, None),
            P(("grp", "far", "near")),
            P(("grp", "bat"), None),
        ),
        out_specs=P(None, ("grp", "bat")),
        check_vma=False,
    )
```

```python
import functools

import jax
import jax.numpy as jnp
from jax import lax
from jax.experimental import pallas as pl
from jax.experimental.pallas import tpu as pltpu
from jax.sharding import Mesh, PartitionSpec as P


F32 = jnp.float32
BF16 = jnp.bfloat16
BLOCK = 4
PREFIX = 4
SHIFT = 1
PARAMS = pltpu.CompilerParams(vmem_limit_bytes=16 * 1024 * 1024)


def lane_sign(rows, width):
    lane = lax.broadcasted_iota(jnp.int32, (rows, width), 1)
    return jnp.where(lane < width // 2, -1.0, 1.0).astype(F32)


def rotated(block, sign):
    return pltpu.roll(block, block.shape[1] // 2, 1) * sign


def split(value):
    high = value.astype(BF16)
    low = (value - high.astype(F32)).astype(BF16)
    return high, low


def dot(a, b):
    return jnp.dot(a, b, preferred_element_type=F32)


def pair_product(first, second, sign):
    width = first.shape[1]
    first_high, first_low = split(first)
    second_high, second_low = split(jnp.concatenate([second, rotated(second, sign)], axis=0))
    half = jnp.concatenate([second_high, second_low], axis=1)
    both = dot(
        jnp.concatenate([first_high, first_low], axis=1),
        jnp.concatenate([half, half], axis=0),
    )
    return both[:, :width] + both[:, width:]


def opening_matrix(left, right, sign):
    bond, _ = left.shape
    left_high, left_low = split(left)
    right_high, right_low = split(right)
    gram = lax.dot_general(
        jnp.concatenate([right_high, right_high, right_low, right_low], axis=0),
        jnp.concatenate([left_high, left_low, left_high, left_low], axis=0),
        (((0,), (0,)), ((), ())),
        preferred_element_type=F32,
    )
    return gram[:bond] + rotated(gram[bond:], sign)


def column_kernel(
    base, order_ref, role_ref, bits_hbm, tensors_hbm, left_hbm, right_hbm, out_ref,
    bits_ref, tensors_ref, left_ref, right_ref, state_ref, table_ref, start_ref, word_ref, words_ref, arrived,
):
    sites, _, bond, width = tensors_ref.shape
    slots = out_ref.shape[0]
    copies = [
        pltpu.make_async_copy(source, target, arrived.at[index])
        for index, (source, target) in enumerate(
            (
                (bits_hbm, bits_ref),
                (tensors_hbm.at[pl.ds(0, PREFIX)], tensors_ref.at[pl.ds(0, PREFIX)]),
                (tensors_hbm.at[pl.ds(PREFIX, sites - PREFIX)], tensors_ref.at[pl.ds(PREFIX, sites - PREFIX)]),
            )
        )
    ]
    for copy in copies:
        copy.start()
    sign = lane_sign(bond, width)
    mask = role_ref[0]
    qubit = lax.broadcasted_iota(jnp.int32, (8, bits_ref.shape[1]), 1)
    place = jnp.zeros(qubit.shape, F32)
    for site in range(sites):
        place = jnp.where(qubit == order_ref[site], float(1 << site), place)
    place = place.astype(BF16)

    def weights(site):
        halves = []
        for value in range(2):
            tensor = tensors_ref[site, value].astype(F32)
            halves.append(jnp.concatenate([tensor, rotated(tensor, sign)], axis=0).astype(BF16))
        half = jnp.concatenate(halves, axis=1)
        return jnp.concatenate([half, half], axis=0)

    copies[0].wait()
    word = lax.dot_general(
        place, bits_ref[...].astype(F32).astype(BF16), (((1,), (1,)), ((), ())), preferred_element_type=F32
    )
    word_ref[...] = jnp.zeros(word_ref.shape, jnp.int32)
    word_ref[:, :word.shape[1]] = word.astype(jnp.int32)
    to_scalars = pltpu.make_async_copy(word_ref, words_ref, arrived.at[len(copies)])
    to_scalars.start()

    copies[1].wait()
    for value in range(2):
        start_ref[value * bond:(value + 1) * bond, :width] = tensors_ref[0, value]
    start_ref[:, width:] = jnp.zeros((2 * bond, width), BF16)

    @pl.when(role_ref[1] == 1)
    def _():
        edges = [
            pltpu.make_async_copy(left_hbm, left_ref, arrived.at[len(copies) + 1]),
            pltpu.make_async_copy(right_hbm, right_ref, arrived.at[len(copies) + 2]),
        ]
        for edge in edges:
            edge.start()
        for edge in edges:
            edge.wait()
        high, low = split(opening_matrix(left_ref[...], right_ref[...], sign))
        both = dot(jnp.concatenate([high, low], axis=1), weights(0))
        high, low = split(jnp.concatenate([both[:, :width], both[:, width:]], axis=0))
        start_ref[:, :width] = high
        start_ref[:, width:] = low

    operand = start_ref[...]
    for site in range(1, PREFIX):
        both = dot(operand, weights(site))
        high, low = split(jnp.concatenate([both[:, :width], both[:, width:]], axis=0))
        operand = jnp.concatenate([high, low], axis=1)
    table_ref[...] = operand
    to_scalars.wait()
    words = [words_ref[0, (base + slot) ^ mask] for slot in range(slots)]
    for slot in range(slots):
        start = pl.multiple_of((words[slot] & ((1 << PREFIX) - 1)) * bond, bond)
        state_ref[slot * bond:(slot + 1) * bond, :] = table_ref[pl.ds(start, bond), :]

    copies[2].wait()
    for site in range(PREFIX, sites):
        matrix = weights(site)
        for start in range(0, slots, BLOCK):
            both = dot(state_ref[start * bond:(start + BLOCK) * bond, :], matrix)
            for slot in range(start, start + BLOCK):
                part = both[(slot - start) * bond:(slot - start + 1) * bond]
                value = jnp.where((words[slot] & (1 << site)) != 0, part[:, width:], part[:, :width])
                if site == sites - 1:
                    out_ref[slot] = value
                else:
                    high, low = split(value)
                    state_ref[slot * bond:(slot + 1) * bond, :width] = high
                    state_ref[slot * bond:(slot + 1) * bond, width:] = low


def column_products(base, slots, order, bits, role, tensors, left, right):
    sites, _, bond, width = tensors.shape
    scalar = pl.BlockSpec(memory_space=pltpu.SMEM)
    far = pl.BlockSpec(memory_space=pltpu.HBM)
    return pl.pallas_call(
        functools.partial(column_kernel, base),
        out_shape=jax.ShapeDtypeStruct((slots, bond, width), F32),
        in_specs=[scalar, scalar, far, far, far, far],
        out_specs=pl.BlockSpec(memory_space=pltpu.VMEM),
        scratch_shapes=[
            pltpu.VMEM(bits.shape, jnp.int32),
            pltpu.VMEM(tensors.shape, BF16),
            pltpu.VMEM((bond, width), F32),
            pltpu.VMEM((bond, width), F32),
            pltpu.VMEM((slots * bond, 2 * width), BF16),
            pltpu.VMEM(((1 << PREFIX) * bond, 2 * width), BF16),
            pltpu.VMEM((2 * bond, 2 * width), BF16),
            pltpu.VMEM((8, width), jnp.int32),
            pltpu.SMEM((8, width), jnp.int32),
            pltpu.SemaphoreType.DMA((6,)),
        ],
        cost_estimate=pl.CostEstimate(
            flops=sites * slots * bond * (2 * width) ** 2, bytes_accessed=slots * bond * width * 8, transcendentals=0
        ),
        compiler_params=PARAMS,
        name="column_products",
    )(order, role, *(pltpu.with_memory_space_constraint(a, pltpu.HBM) for a in (bits, tensors, left, right)))


def joined(flag, kept, received, sign):
    before = jnp.where(flag, received, kept)
    after = jnp.where(flag, kept, received)
    return pair_product(before, after, sign)


def join_kernel(role_ref, kept_ref, received_ref, *out_refs):
    items, bond, width = kept_ref.shape
    sign = lane_sign(bond, width)
    flag = role_ref[0] == 1
    per = out_refs[0].shape[0]
    for item in range(items):
        out_refs[item // per][item % per] = joined(flag, kept_ref[item], received_ref[item], sign)


def join(flag, kept, received, outs):
    items, bond, width = kept.shape
    out = jax.ShapeDtypeStruct((items // outs, bond, width), F32)
    vector = pl.BlockSpec(memory_space=pltpu.VMEM)
    return pl.pallas_call(
        join_kernel,
        out_shape=(out,) * outs,
        in_specs=[pl.BlockSpec(memory_space=pltpu.SMEM), vector, vector],
        out_specs=(vector,) * outs,
        compiler_params=PARAMS,
        name="join",
    )(flag, kept, received)


def close_kernel(role_ref, opened_ref, kept_ref, received_ref, out_ref):
    items, bond, width = kept_ref.shape
    sign = lane_sign(bond, width)
    row = lax.broadcasted_iota(jnp.int32, (bond, width), 0)
    lane = lax.broadcasted_iota(jnp.int32, (bond, width), 1)
    slot = lax.broadcasted_iota(jnp.int32, out_ref.shape, 1)
    which = lax.broadcasted_iota(jnp.int32, out_ref.shape, 0)
    flag = role_ref[1] == 1
    late = role_ref[2] == 1
    total = jnp.zeros(out_ref.shape, F32)
    for item in range(items):
        end = joined(flag, kept_ref[item], received_ref[item], sign)
        whole = pair_product(opened_ref[item], end, sign)
        real = jnp.sum(jnp.where(row == lane, whole, 0.0), keepdims=True)
        imag = jnp.sum(jnp.where(row + bond == lane, whole, 0.0), keepdims=True)
        value = jnp.where(which == 0, real, imag)
        total = jnp.where(slot == (role_ref[0] ^ item), value, total)
    out_ref[...] = jnp.where(late, total, 0.0)


def close(base, opened, kept, received, rows):
    vector = pl.BlockSpec(memory_space=pltpu.VMEM)
    return pl.pallas_call(
        close_kernel,
        out_shape=jax.ShapeDtypeStruct((2, rows), F32),
        in_specs=[pl.BlockSpec(memory_space=pltpu.SMEM), vector, vector, vector],
        out_specs=vector,
        compiler_params=PARAMS,
        name="close",
    )(base, opened, kept, received)


AXES = ("far", "near", "bat")


def pairs(cols, cores, target):
    found = []
    for core in range(cores):
        for role in range(cols):
            other = target(role)
            if other is not None:
                found.append(((role + SHIFT * core) % cols * cores + core, (other + SHIFT * core) % cols * cores + core))
    return found


def solution(mesh):
    shape = dict(mesh.shape)
    inner = 4
    outer = shape["col"] // inner
    cores = shape["bat"]
    cols = shape["col"]
    half, quarter = cols // 2, cols // 4
    fine = Mesh(
        mesh.devices.reshape(shape["grp"], outer, inner, shape["slc"], cores),
        ("grp", "far", "near", "slc", "bat"),
    )

    def swap(distance, late):
        return pairs(cols, cores, lambda role: role ^ distance if (role >= half) == late else None)

    def on_device(site_tensors, left_edge, right_edge, order, bitstrings):
        rows = bitstrings.shape[0]
        core = lax.axis_index("bat")
        col = lax.axis_index("far") * inner + lax.axis_index("near")
        role = (col - SHIFT * core + cols) % cols
        bit0, bit1, bit2, late = role & 1, (role >> 1) & 1, (role >> 2) & 1, (role >> 3) & 1
        mask = bit0 * (rows // 2) + bit1 * (rows // 4) + (bit2 ^ late) * (rows // 8)
        first = (col == 0).astype(jnp.int32)
        operands = (order, bitstrings, jnp.stack([mask, first]), site_tensors[0], left_edge[0], right_edge[0])
        sent = column_products(rows // 2, rows // 2, *operands)
        kept = column_products(0, rows // 2, *operands)

        def move(value, found):
            return lax.ppermute(value, AXES, found)

        def quads(late):
            received = move(sent, swap(1, late))
            stay, leave = join(bit0[None], kept, received, 2)
            received = move(leave, swap(2, late))
            return join(bit1[None], stay, received, 2)

        stay, leave = quads(False)
        received = move(leave, swap(quarter, False))
        (early,) = join(bit2[None], stay, received, 1)
        across = pairs(cols, cores, lambda role: (role ^ quarter) + half if role < half else None)
        opened = move(early, across)
        stay, leave = quads(True)
        received = move(leave, swap(quarter, True))
        placed = close(jnp.stack([mask, bit2, late]), opened, stay, received, rows)
        everyone = outer * inner * shape["slc"]
        spread = jnp.broadcast_to(placed, (everyone, 2, rows))
        gathered = lax.all_to_all(spread, ("far", "near", "slc"), split_axis=0, concat_axis=0, tiled=True)
        return jnp.sum(gathered, axis=0)

    return jax.shard_map(
        on_device,
        mesh=fine,
        in_specs=(
            P(("grp", "slc"), ("far", "near"), None, None, None),
            P(("grp", "slc"), None, None),
            P(("grp", "slc"), None, None),
            P(("grp", "far", "near")),
            P(("grp", "bat"), None),
        ),
        out_specs=P(None, ("grp", "bat")),
        check_vma=False,
    )
```

```python
import functools

import jax
import jax.numpy as jnp
from jax import lax
from jax.experimental import pallas as pl
from jax.experimental.pallas import tpu as pltpu
from jax.sharding import Mesh, PartitionSpec as P


F32 = jnp.float32
BF16 = jnp.bfloat16
BLOCK = 4
PREFIX = 4
SHIFT = 1
PARAMS = pltpu.CompilerParams(vmem_limit_bytes=16 * 1024 * 1024)


def lane_sign(rows, width):
    lane = lax.broadcasted_iota(jnp.int32, (rows, width), 1)
    return jnp.where(lane < width // 2, -1.0, 1.0).astype(F32)


def rotated(block, sign):
    return pltpu.roll(block, block.shape[1] // 2, 1) * sign


def split(value):
    high = value.astype(BF16)
    low = (value - high.astype(F32)).astype(BF16)
    return high, low


def dot(a, b):
    return jnp.dot(a, b, preferred_element_type=F32)


def pair_product(first, second, sign):
    width = first.shape[1]
    first_high, first_low = split(first)
    second_high, second_low = split(jnp.concatenate([second, rotated(second, sign)], axis=0))
    half = jnp.concatenate([second_high, second_low], axis=1)
    both = dot(
        jnp.concatenate([first_high, first_low], axis=1),
        jnp.concatenate([half, half], axis=0),
    )
    return both[:, :width] + both[:, width:]


def opening_matrix(left, right, sign):
    bond, _ = left.shape
    left_high, left_low = split(left)
    right_high, right_low = split(right)
    gram = lax.dot_general(
        jnp.concatenate([right_high, right_high, right_low, right_low], axis=0),
        jnp.concatenate([left_high, left_low, left_high, left_low], axis=0),
        (((0,), (0,)), ((), ())),
        preferred_element_type=F32,
    )
    return gram[:bond] + rotated(gram[bond:], sign)


def column_kernel(
    base, order_ref, role_ref, bits_hbm, tensors_hbm, left_hbm, right_hbm, out_ref,
    bits_ref, tensors_ref, left_ref, right_ref, state_ref, table_ref, start_ref, word_ref, words_ref, arrived,
):
    sites, _, bond, width = tensors_ref.shape
    slots = out_ref.shape[0]
    copies = [
        pltpu.make_async_copy(source, target, arrived.at[index])
        for index, (source, target) in enumerate(
            (
                (bits_hbm, bits_ref),
                (tensors_hbm.at[pl.ds(0, PREFIX)], tensors_ref.at[pl.ds(0, PREFIX)]),
                (tensors_hbm.at[pl.ds(PREFIX, sites - PREFIX)], tensors_ref.at[pl.ds(PREFIX, sites - PREFIX)]),
            )
        )
    ]
    for copy in copies:
        copy.start()
    sign = lane_sign(bond, width)
    mask = role_ref[0]
    qubit = lax.broadcasted_iota(jnp.int32, (8, bits_ref.shape[1]), 1)
    place = jnp.zeros(qubit.shape, F32)
    for site in range(sites):
        place = jnp.where(qubit == order_ref[site], float(1 << site), place)
    place = place.astype(BF16)

    def weights(site):
        halves = []
        for value in range(2):
            tensor = tensors_ref[site, value].astype(F32)
            halves.append(jnp.concatenate([tensor, rotated(tensor, sign)], axis=0).astype(BF16))
        half = jnp.concatenate(halves, axis=1)
        return jnp.concatenate([half, half], axis=0)

    copies[0].wait()
    word = lax.dot_general(
        place, bits_ref[...].astype(F32).astype(BF16), (((1,), (1,)), ((), ())), preferred_element_type=F32
    )
    word_ref[...] = jnp.zeros(word_ref.shape, jnp.int32)
    word_ref[:, :word.shape[1]] = word.astype(jnp.int32)
    to_scalars = pltpu.make_async_copy(word_ref, words_ref, arrived.at[len(copies)])
    to_scalars.start()

    copies[1].wait()
    for value in range(2):
        start_ref[value * bond:(value + 1) * bond, :width] = tensors_ref[0, value]
    start_ref[:, width:] = jnp.zeros((2 * bond, width), BF16)

    @pl.when(role_ref[1] == 1)
    def _():
        edges = [
            pltpu.make_async_copy(left_hbm, left_ref, arrived.at[len(copies) + 1]),
            pltpu.make_async_copy(right_hbm, right_ref, arrived.at[len(copies) + 2]),
        ]
        for edge in edges:
            edge.start()
        for edge in edges:
            edge.wait()
        high, low = split(opening_matrix(left_ref[...], right_ref[...], sign))
        both = dot(jnp.concatenate([high, low], axis=1), weights(0))
        high, low = split(jnp.concatenate([both[:, :width], both[:, width:]], axis=0))
        start_ref[:, :width] = high
        start_ref[:, width:] = low

    operand = start_ref[...]
    for site in range(1, PREFIX):
        both = dot(operand, weights(site))
        high, low = split(jnp.concatenate([both[:, :width], both[:, width:]], axis=0))
        operand = jnp.concatenate([high, low], axis=1)
    table_ref[...] = operand
    to_scalars.wait()
    words = [words_ref[0, (base + slot) ^ mask] for slot in range(slots)]
    for slot in range(slots):
        start = pl.multiple_of((words[slot] & ((1 << PREFIX) - 1)) * bond, bond)
        state_ref[slot * bond:(slot + 1) * bond, :] = table_ref[pl.ds(start, bond), :]

    copies[2].wait()
    for site in range(PREFIX, sites):
        matrix = weights(site)
        for start in range(0, slots, BLOCK):
            both = dot(state_ref[start * bond:(start + BLOCK) * bond, :], matrix)
            for slot in range(start, start + BLOCK):
                part = both[(slot - start) * bond:(slot - start + 1) * bond]
                value = jnp.where((words[slot] & (1 << site)) != 0, part[:, width:], part[:, :width])
                if site == sites - 1:
                    out_ref[slot] = value
                else:
                    high, low = split(value)
                    state_ref[slot * bond:(slot + 1) * bond, :width] = high
                    state_ref[slot * bond:(slot + 1) * bond, width:] = low


def column_products(base, slots, order, bits, role, tensors, left, right):
    sites, _, bond, width = tensors.shape
    scalar = pl.BlockSpec(memory_space=pltpu.SMEM)
    far = pl.BlockSpec(memory_space=pltpu.HBM)
    return pl.pallas_call(
        functools.partial(column_kernel, base),
        out_shape=jax.ShapeDtypeStruct((slots, bond, width), F32),
        in_specs=[scalar, scalar, far, far, far, far],
        out_specs=pl.BlockSpec(memory_space=pltpu.VMEM),
        scratch_shapes=[
            pltpu.VMEM(bits.shape, jnp.int32),
            pltpu.VMEM(tensors.shape, BF16),
            pltpu.VMEM((bond, width), F32),
            pltpu.VMEM((bond, width), F32),
            pltpu.VMEM((slots * bond, 2 * width), BF16),
            pltpu.VMEM(((1 << PREFIX) * bond, 2 * width), BF16),
            pltpu.VMEM((2 * bond, 2 * width), BF16),
            pltpu.VMEM((8, width), jnp.int32),
            pltpu.SMEM((8, width), jnp.int32),
            pltpu.SemaphoreType.DMA((6,)),
        ],
        cost_estimate=pl.CostEstimate(
            flops=sites * slots * bond * (2 * width) ** 2, bytes_accessed=slots * bond * width * 8, transcendentals=0
        ),
        compiler_params=PARAMS,
        name="column_products",
    )(order, role, *(pltpu.with_memory_space_constraint(a, pltpu.HBM) for a in (bits, tensors, left, right)))


def joined(flag, kept, received, sign):
    before = jnp.where(flag, received, kept)
    after = jnp.where(flag, kept, received)
    return pair_product(before, after, sign)


def join_kernel(role_ref, kept_ref, received_ref, *out_refs):
    items, bond, width = kept_ref.shape
    sign = lane_sign(bond, width)
    flag = role_ref[0] == 1
    per = out_refs[0].shape[0]
    for item in range(items):
        out_refs[item // per][item % per] = joined(flag, kept_ref[item], received_ref[item], sign)


def join(flag, kept, received, outs):
    items, bond, width = kept.shape
    out = jax.ShapeDtypeStruct((items // outs, bond, width), F32)
    vector = pl.BlockSpec(memory_space=pltpu.VMEM)
    return pl.pallas_call(
        join_kernel,
        out_shape=(out,) * outs,
        in_specs=[pl.BlockSpec(memory_space=pltpu.SMEM), vector, vector],
        out_specs=(vector,) * outs,
        compiler_params=PARAMS,
        name="join",
    )(flag, kept, received)


def close_kernel(role_ref, opened_ref, received_ref, out_ref):
    items, bond, width = received_ref.shape
    sign = lane_sign(bond, width)
    row = lax.broadcasted_iota(jnp.int32, (bond, width), 0)
    lane = lax.broadcasted_iota(jnp.int32, (bond, width), 1)
    slot = lax.broadcasted_iota(jnp.int32, out_ref.shape, 1)
    which = lax.broadcasted_iota(jnp.int32, out_ref.shape, 0)
    total = jnp.zeros(out_ref.shape, F32)
    for item in range(items):
        whole = pair_product(opened_ref[item], received_ref[item], sign)
        real = jnp.sum(jnp.where(row == lane, whole, 0.0), keepdims=True)
        imag = jnp.sum(jnp.where(row + bond == lane, whole, 0.0), keepdims=True)
        value = jnp.where(which == 0, real, imag)
        total = jnp.where(slot == (role_ref[0] ^ item), value, total)
    out_ref[...] = jnp.where(role_ref[1] == 1, total, 0.0)


def close(base, opened, received, rows):
    vector = pl.BlockSpec(memory_space=pltpu.VMEM)
    return pl.pallas_call(
        close_kernel,
        out_shape=jax.ShapeDtypeStruct((2, rows), F32),
        in_specs=[pl.BlockSpec(memory_space=pltpu.SMEM), vector, vector],
        out_specs=vector,
        compiler_params=PARAMS,
        name="close",
    )(base, opened, received)


AXES = ("far", "near", "bat")


def pairs(cols, cores, target):
    found = []
    for core in range(cores):
        for role in range(cols):
            other = target(role)
            if other is not None:
                found.append(((role + SHIFT * core) % cols * cores + core, (other + SHIFT * core) % cols * cores + core))
    return found


def solution(mesh):
    shape = dict(mesh.shape)
    inner = 4
    outer = shape["col"] // inner
    cores = shape["bat"]
    cols = shape["col"]
    half, quarter = cols // 2, cols // 4
    fine = Mesh(
        mesh.devices.reshape(shape["grp"], outer, inner, shape["slc"], cores),
        ("grp", "far", "near", "slc", "bat"),
    )

    def swap(distance, late):
        return pairs(cols, cores, lambda role: role ^ distance if (role >= half) == late else None)

    def on_device(site_tensors, left_edge, right_edge, order, bitstrings):
        rows = bitstrings.shape[0]
        core = lax.axis_index("bat")
        col = lax.axis_index("far") * inner + lax.axis_index("near")
        role = (col - SHIFT * core + cols) % cols
        bit0, bit1, bit2, late = role & 1, (role >> 1) & 1, (role >> 2) & 1, (role >> 3) & 1
        mask = bit0 * (rows // 2) + bit1 * (rows // 4) + (bit2 ^ late) * (rows // 8)
        first = (col == 0).astype(jnp.int32)
        operands = (order, bitstrings, jnp.stack([mask, first]), site_tensors[0], left_edge[0], right_edge[0])
        sent = column_products(rows // 2, rows // 2, *operands)
        kept = column_products(0, rows // 2, *operands)

        def move(value, found):
            return lax.ppermute(value, AXES, found)

        def quads(late):
            received = move(sent, swap(1, late))
            stay, leave = join(bit0[None], kept, received, 2)
            received = move(leave, swap(2, late))
            return join(bit1[None], stay, received, 2)

        stay, leave = quads(False)
        received = move(leave, swap(quarter, False))
        (early,) = join(bit2[None], stay, received, 1)
        across = pairs(cols, cores, lambda role: (role ^ quarter) + half if role < half else None)
        opened = move(early, across)
        stay, leave = quads(True)
        received = move(leave, swap(quarter, True))
        (opened,) = join(bit2[None], opened, stay, 1)
        placed = close(jnp.stack([mask, late]), opened, received, rows)
        everyone = outer * inner * shape["slc"]
        spread = jnp.broadcast_to(placed, (everyone, 2, rows))
        gathered = lax.all_to_all(spread, ("far", "near", "slc"), split_axis=0, concat_axis=0, tiled=True)
        return jnp.sum(gathered, axis=0)

    return jax.shard_map(
        on_device,
        mesh=fine,
        in_specs=(
            P(("grp", "slc"), ("far", "near"), None, None, None),
            P(("grp", "slc"), None, None),
            P(("grp", "slc"), None, None),
            P(("grp", "far", "near")),
            P(("grp", "bat"), None),
        ),
        out_specs=P(None, ("grp", "bat")),
        check_vma=False,
    )
```
